32 devices in a mesh: src: 8 (over z, x), grp: 4 (over y, core).
Axes of the slice: x: 2, y: 2, z: 4, core: 2. Of those that a mesh axis runs over, the one named last changes fastest.
Arguments:
- currents: bfloat16 [65536, 1024], P(('src', 'grp')), may hold values from -6 to 6
- leaf_basis: bfloat16 [2, 40, 65536], P(None, None, ('src', 'grp')), may hold values from -6 to 6
- leaf_box: int32 [65536], P(('src', 'grp')), may hold values from 0 to 7, as said below
- box_count: int32 [256], P(('src', 'grp')), may hold values from 1 to 2041, as said below
- merge_factor: bfloat16 [2, 320, 10240], P(None, None, ('src', 'grp')), may hold values from -0.25 to 0.25
- angle_factor: bfloat16 [512, 4, 2, 320], P('src'), may hold values from -0.125 to 0.125
Outputs:
- normalized: float32 [512, 512], P('src', 'grp')
- peak_value: float32 [512], P('grp')
The draws below stay inside these ranges and needn't reach their ends.
Inputs may be any that keep to these rules, and one draw needn't show every extreme that they name: `leaf_box`: every source block of 2048 currents holds one or more currents of each of its 8 leaf boxes; some blocks put all but 7 of their currents into one box. box_count[k * 8 + b] is the number of currents of source block k whose leaf_box is b.
All inputs are finite; a program needn't handle non-finite values.
Results may differ from the reference program's by a relative error of at most 0.0057.
Values may be sent and summed in bfloat16 or wider, within the bound.
A program may use at most 128 MiB of HBM per device.

```python
import jax
import jax.numpy as jnp
from jax import lax

R = 40
S_DEV = 2048
NE = 512
LEAF = 8
A_DEV = 64
S = 65536
LEAVES = 256
NA = 512
N_SRC = 8
N_GRP = 4


def leaf_layout(key):
    blocks = S // S_DEV
    position = jnp.arange(S_DEV, dtype=jnp.int32)[None, :]
    block_ids = jnp.arange(blocks, dtype=jnp.int32)[:, None]
    first_pick = jax.random.randint(jax.random.fold_in(key, 7), (blocks, S_DEV), 0, LEAF)
    second_pick = jax.random.randint(jax.random.fold_in(key, 11), (blocks, S_DEV), 0, LEAF)
    chosen = jnp.minimum(first_pick, second_pick).astype(jnp.int32)
    lone_box = jax.random.randint(jax.random.fold_in(key, 13), (blocks, 1), 0, LEAF).astype(jnp.int32)
    crowded = block_ids % 16 == 0
    chosen = jnp.where(crowded, lone_box, chosen).astype(jnp.int32)
    return jnp.where(position < LEAF, position, chosen).astype(jnp.int32)


def draw_leaf_box(key, part):
    return leaf_layout(key).reshape(S)


def draw_box_count(key, part):
    layout = leaf_layout(key)
    labels = jnp.arange(LEAF, dtype=jnp.int32)
    tallies = jnp.sum((layout[:, None, :] == labels[None, :, None]).astype(jnp.int32), axis=2)
    return tallies.reshape(LEAVES).astype(jnp.int32)


def level_of(rng, shape, pieces, least, largest):
    def one(dim, shards_of):
        draws = jax.random.uniform(jax.random.fold_in(jax.random.fold_in(rng, 6), dim), (shards_of,), jnp.float32, least / len(pieces), largest / len(pieces))
        return jnp.repeat(jnp.exp(draws), shape[dim] // shards_of).reshape((-1,) + (1,) * (len(shape) - dim - 1))

    level = one(*pieces[0])
    for cut in pieces[1:]:
        level = level * one(*cut)
    return level


def centred(own_key, dims, spread, limit, cuts=(), kind=jnp.bfloat16):
    result = spread * jax.random.normal(own_key, dims, jnp.float32)
    if cuts:
        result = result * level_of(own_key, dims, cuts, -0.22, 0.18)
    return jnp.clip(result, -limit, limit).astype(kind)


def setup_inputs(seed: int = 0) -> dict:
    splits = jax.random.split(jax.random.key(seed), 7)
    currents = centred(splits[0], (S, 2 * NE), 1.0, 6.0, ((0, 32),))
    leaf_basis = centred(splits[1], (2, R, S), 1.0, 6.0, ((2, 32),))
    leaf_box = draw_leaf_box(jax.random.fold_in(splits[6], 71), 0)
    box_count = draw_box_count(jax.random.fold_in(splits[6], 71), 0)
    merge_factor = centred(splits[4], (2, N_SRC * R, LEAVES * R), (2 * LEAF * R) ** -0.5, 0.25, ((2, 32),))
    angle_factor = centred(splits[5], (NA, N_GRP, 2, N_SRC * R), (2 * N_SRC * N_GRP * R) ** -0.5, 0.125, ((0, 8),))
    return dict(currents=currents, leaf_basis=leaf_basis, leaf_box=leaf_box, box_count=box_count, merge_factor=merge_factor, angle_factor=angle_factor)


def complex_apply(real_part, imag_part, right_side):
    half_width = right_side.shape[1] // 2
    first_part = jnp.dot(real_part, right_side, preferred_element_type=jnp.float32)
    second = jnp.dot(imag_part, right_side, preferred_element_type=jnp.float32)
    return jnp.concatenate([first_part[:, :half_width] - second[:, half_width:], first_part[:, half_width:] + second[:, :half_width]], axis=1)

def source_coefs(currents, leaf_basis, leaf_box, box_count, merge_factor):
    leaf_total = box_count.shape[0]
    rank_size = leaf_basis.shape[1]
    sources = currents.shape[0]
    labels = jnp.arange(leaf_total, dtype=jnp.int32)
    member = (leaf_box[None, :] == labels[:, None]).astype(jnp.float32)
    scaled = member * lax.rsqrt(box_count.astype(jnp.float32))[:, None]
    basis_wide = leaf_basis.astype(jnp.float32)
    left_real = (scaled[:, None, :] * basis_wide[0][None, :, :]).reshape(leaf_total * rank_size, sources).astype(jnp.bfloat16)
    left_imag = (scaled[:, None, :] * basis_wide[1][None, :, :]).reshape(leaf_total * rank_size, sources).astype(jnp.bfloat16)
    leaf_coefs = complex_apply(left_real, left_imag, currents).astype(jnp.bfloat16)
    return complex_apply(merge_factor[0], merge_factor[1], leaf_coefs).astype(jnp.bfloat16)

def angle_side(operands):
    factor, level_coefs = operands
    half_width = level_coefs.shape[2] // 2
    wide_coefs = level_coefs.astype(jnp.float32)
    first_part = jnp.einsum('aqk,qkc->ac', factor[:, :, 0].astype(jnp.float32), wide_coefs)
    second = jnp.einsum('aqk,qkc->ac', factor[:, :, 1].astype(jnp.float32), wide_coefs)
    return jnp.stack([first_part[:, :half_width] - second[:, half_width:], first_part[:, half_width:] + second[:, :half_width]], axis=1)

def reference(currents, leaf_basis, leaf_box, box_count, merge_factor, angle_factor):
    blocks = N_SRC * N_GRP
    rank_size = leaf_basis.shape[1]
    width_cols = currents.shape[1]

    def source_block(block_index):
        first_row = (block_index * S_DEV).astype(jnp.int32)
        first_leaf = (block_index * LEAF).astype(jnp.int32)
        block_currents = lax.dynamic_slice_in_dim(currents, first_row, S_DEV, 0)
        block_basis = lax.dynamic_slice_in_dim(leaf_basis, first_row, S_DEV, 2)
        block_boxes = lax.dynamic_slice_in_dim(leaf_box, first_row, S_DEV, 0)
        block_counts = lax.dynamic_slice_in_dim(box_count, first_leaf, LEAF, 0)
        block_merge = lax.dynamic_slice_in_dim(merge_factor, (first_leaf * rank_size).astype(jnp.int32), LEAF * rank_size, 2)
        return source_coefs(block_currents, block_basis, block_boxes, block_counts, block_merge)
    all_coefs = lax.map(source_block, jnp.arange(blocks, dtype=jnp.int32))
    grouped = all_coefs.reshape(N_SRC, N_GRP, N_SRC, rank_size, width_cols)
    grouped = grouped.transpose(2, 1, 0, 3, 4).reshape(N_SRC, N_GRP, N_SRC * rank_size, width_cols)
    factors = angle_factor.reshape(N_SRC, A_DEV, N_GRP, 2, N_SRC * rank_size)
    patterns = lax.map(angle_side, (factors, grouped))
    pattern = patterns.reshape(N_SRC * A_DEV, 2, width_cols // 2)
    intensity = pattern[:, 0] * pattern[:, 0] + pattern[:, 1] * pattern[:, 1]
    peak_value = lax.optimization_barrier(jnp.max(intensity, axis=0))
    return (intensity / (peak_value[None, :] + 1.0), peak_value)
```

```python
import functools
import math

import jax
import jax.numpy as jnp
from jax import lax
from jax.experimental import pallas as pl
from jax.experimental.pallas import tpu as pltpu
from jax.sharding import PartitionSpec as P

MESH = pl.DeviceIdType.MESH
F32 = jnp.float32
BF16 = jnp.bfloat16


def kernel(
    planes, lanes, parties, halves, count_hbm, box_hbm, basis_hbm, currents_hbm, merge_hbm, angle_hbm,
    out_ref, peak_ref,
    count_ref, box_ref, basis, x, merge, angle, left, outgoing, received, factor_out, factor_in, part_out, part_in,
    peaks,
    load_sem, x_sem, send_sem, recv_sem, factor_send, factor_recv, forward_send, part_send, part_recv, peak_send,
    peak_recv,
):
    me = lax.axis_index("src")
    my_plane, my_lane = me // lanes, lax.rem(me, lanes)
    my_party = lax.axis_index("grp")
    my_half = lax.rem(my_party, halves)
    partner = my_party + (halves - 1) * (1 - 2 * my_half)
    groups = planes * lanes
    peers = lanes * parties
    rank = merge.shape[1] // groups
    leaves = count_ref.shape[0]
    share = x.shape[2] // 2
    excite = currents_hbm.shape[1] // 2
    some = angle.shape[0]
    angles = some * halves
    split = 2 if leaves % 2 == 0 else 1
    unroll = planes <= 8

    load_angle = pltpu.make_async_copy(angle_hbm.at[pl.ds(my_half * some, some)], angle, load_sem.at[0])
    load_angle.start()
    load_basis = pltpu.make_async_copy(basis_hbm, basis, load_sem.at[1])
    load_basis.start()
    load_box = pltpu.make_async_copy(box_hbm, box_ref, load_sem.at[2])
    load_box.start()
    load_count = pltpu.make_async_copy(count_hbm, count_ref, load_sem.at[3])
    load_count.start()
    loads = []
    for step in range(parties):
        quarter = lax.rem(my_party + 1 + step, parties)
        pair = []
        for part in range(2):
            start = pl.multiple_of(part * excite + quarter * share, 128)
            copy = pltpu.make_async_copy(
                currents_hbm.at[:, pl.ds(start, share)],
                x.at[step, :, pl.ds(part * share, share)],
                x_sem.at[step, part],
            )
            copy.start()
            pair.append(copy)
        loads.append(pair)
        if step == 0:
            load_merge = pltpu.make_async_copy(merge_hbm, merge, load_sem.at[4])
            load_merge.start()

    barrier = pltpu.get_barrier_semaphore()

    def peer(i):
        other = lax.rem(my_lane * parties + my_party + i, peers)
        return other // parties, lax.rem(other, parties)

    def greet(i, carry):
        lane, party = peer(i)
        pl.semaphore_signal(
            barrier, inc=1, device_id=(my_plane * lanes + lane, party), device_id_type=MESH
        )
        return carry

    lax.fori_loop(1, peers, greet, 0)

    def greet_far(i, carry):
        plane = lax.rem(my_plane + 1 + i // lanes, planes)
        pl.semaphore_signal(
            barrier,
            inc=1,
            device_id=(plane * lanes + lax.rem(i, lanes), my_party),
            device_id_type=MESH,
        )
        return carry

    lax.fori_loop(0, (planes - 1) * lanes, greet_far, 0)

    def remote(i):
        upper = lax.rem(my_plane // ((planes + 1) // 2), 2)
        down = planes - 1 - i
        down = down - (my_plane - down + planes) // planes
        up = i + (i - my_plane + planes) // planes
        return (1 - upper) * down + upper * up

    with jax.named_scope("factor_build"):
        load_angle.wait()
        wide = [angle[:, q].astype(F32) for q in range(parties)]
        span = lanes * rank
        for h in range(planes):
            rows = [
                jnp.concatenate([wide[q][:, p, h * span : (h + 1) * span] for q in range(parties)], axis=1)
                for p in range(2)
            ]
            factor_out[h] = jnp.concatenate(rows, axis=0).astype(BF16)

    with jax.named_scope("barrier"):
        pl.semaphore_wait(barrier, peers - 1 + (planes - 1) * lanes)

    def share_factor(i, carry):
        h = remote(i)
        pltpu.make_async_remote_copy(
            src_ref=factor_out.at[h],
            dst_ref=factor_in.at[my_plane, my_half],
            send_sem=factor_send.at[h],
            recv_sem=factor_recv.at[my_plane, my_half],
            device_id=(h * lanes + my_lane, my_party),
            device_id_type=MESH,
        ).start()
        return carry

    lax.fori_loop(0, planes - 1, share_factor, 0)
    if halves > 1:
        pltpu.make_async_remote_copy(
            src_ref=factor_out.at[my_plane],
            dst_ref=factor_in.at[my_plane, my_half],
            send_sem=factor_send.at[my_plane],
            recv_sem=factor_recv.at[my_plane, my_half],
            device_id=(me, partner),
            device_id_type=MESH,
        ).start()
    factor_in[my_plane, my_half] = factor_out[my_plane]

    with jax.named_scope("left_build"):
        load_box.wait()
        load_count.wait()
        box = box_ref[...]
        count = jnp.zeros(box.shape, F32)
        for b in range(leaves):
            count = jnp.where(box == b, count_ref[b].astype(F32), count)
        scale = lax.rsqrt(jnp.maximum(count, 1.0))
        load_basis.wait()
        scaled = (basis[...].astype(F32) * scale).astype(BF16)
        for b in range(leaves):
            member = (box == b).astype(F32).astype(BF16)
            left[2 * rank * b : 2 * rank * (b + 1), :] = scaled * member

    def send(step, lane, plane):
        quarter = lax.rem(my_party + 1 + step, parties)
        pltpu.make_async_remote_copy(
            src_ref=outgoing.at[step, lane, plane],
            dst_ref=received.at[my_party, my_lane, plane],
            send_sem=send_sem.at[step, lane, plane],
            recv_sem=recv_sem.at[my_party, my_lane, plane],
            device_id=(my_plane * lanes + lane, quarter),
            device_id_type=MESH,
        ).start()

    block = math.gcd(groups, 8)
    for step in range(parties):
        with jax.named_scope(f"xwait{step}"):
            for copy in loads[step]:
                copy.wait()
        with jax.named_scope(f"leaf{step}"):
            chunks = []
            depth = leaves // split
            for c in range(split):
                rows = slice(2 * rank * depth * c, 2 * rank * depth * (c + 1))
                raw = jnp.dot(left[rows, :], x[step], preferred_element_type=F32)
                reals, imags = [], []
                for b in range(depth):
                    top = raw[2 * rank * b : 2 * rank * b + rank]
                    low = raw[2 * rank * b + rank : 2 * rank * (b + 1)]
                    reals.append(top[:, :share] - low[:, share:])
                    imags.append(top[:, share:] + low[:, :share])
                chunks.append(
                    jnp.concatenate(
                        [jnp.concatenate(reals, axis=0), jnp.concatenate(imags, axis=0)], axis=1
                    )
                )
            leaf = jnp.concatenate(chunks, axis=0).astype(BF16)
        with jax.named_scope(f"merge{step}"):
            if step == 0:
                load_merge.wait()
            for first in range(0, groups, block):
                rows = slice(first * rank, (first + block) * rank)
                one = jnp.dot(merge[0, rows, :], leaf, preferred_element_type=F32)
                two = jnp.dot(merge[1, rows, :], leaf, preferred_element_type=F32)
                real = (one[:, :share] - two[:, share:]).astype(BF16)
                imag = (one[:, share:] + two[:, :share]).astype(BF16)
                for g in range(block):
                    cut = slice(g * rank, (g + 1) * rank)
                    plane, lane = divmod(first + g, lanes)
                    outgoing[step, lane, plane, :rank] = real[cut]
                    outgoing[step, lane, plane, rank:] = imag[cut]
        own = 1 if step == parties - 1 else 0

        def send_plane(i, carry):
            plane = remote(i)

            def send_lane(j, inner):
                send(step, lax.rem(my_lane + j, lanes), plane)
                return inner

            return lax.fori_loop(own, lanes, send_lane, carry)

        lax.fori_loop(0, planes - 1, send_plane, 0)

    for step in range(parties):

        def send_home(j, carry):
            send(step, lax.rem(my_lane + j, lanes), my_plane)
            return carry

        lax.fori_loop(1 if step == parties - 1 else 0, lanes, send_home, 0)
    received[my_party, my_lane] = outgoing[parties - 1, my_lane]

    with jax.named_scope("forward"):

        def forward(i, carry):
            h = remote(planes - 2 - i)
            pltpu.make_async_copy(
                factor_in.at[h, my_half], factor_in.at[h, my_half], factor_recv.at[h, my_half]
            ).wait()
            if halves > 1:
                pltpu.make_async_remote_copy(
                    src_ref=factor_in.at[h, my_half],
                    dst_ref=factor_in.at[h, my_half],
                    send_sem=forward_send.at[h],
                    recv_sem=factor_recv.at[h, my_half],
                    device_id=(me, partner),
                    device_id_type=MESH,
                ).start()
            return carry

        lax.fori_loop(0, planes - 1, forward, 0)

    def factor_ready(h):
        if halves > 1:
            other = factor_in.at[h, 1 - my_half]
            pltpu.make_async_copy(other, other, factor_recv.at[h, 1 - my_half]).wait()

    def arrived(h):
        def arrive(i, carry):
            lane, party = peer(i)
            piece = received.at[party, lane, h]
            pltpu.make_async_copy(piece, piece, recv_sem.at[party, lane, h]).wait()
            return carry

        lax.fori_loop(1, peers, arrive, 0)

    def partial(h):
        pieces = [
            received[q, lane, h].astype(F32) for q in range(parties) for lane in range(lanes)
        ]
        coefs = jnp.concatenate(
            [
                jnp.concatenate([piece[:rank] for piece in pieces], axis=0),
                jnp.concatenate([piece[rank:] for piece in pieces], axis=0),
            ],
            axis=1,
        ).astype(BF16)
        reals, imags = [], []
        total = jnp.dot(factor_in[h].reshape(2 * angles, -1), coefs, preferred_element_type=F32)
        for k in range(halves):
            top = total[2 * some * k : 2 * some * k + some]
            low = total[2 * some * k + some : 2 * some * (k + 1)]
            reals.append(top[:, :share] - low[:, share:])
            imags.append(top[:, share:] + low[:, :share])
        return jnp.concatenate(
            [jnp.concatenate(reals, axis=0), jnp.concatenate(imags, axis=0)], axis=1
        )

    def pass_on(i, carry):
        h = remote(i)
        factor_ready(h)
        arrived(h)
        part_out[h] = partial(h).astype(BF16)
        pltpu.make_async_remote_copy(
            src_ref=part_out.at[h],
            dst_ref=part_in.at[my_plane],
            send_sem=part_send.at[h],
            recv_sem=part_recv.at[my_plane],
            device_id=(h * lanes + my_lane, my_party),
            device_id_type=MESH,
        ).start()
        return carry

    with jax.named_scope("pass_on"):
        lax.fori_loop(0, planes - 1, pass_on, 0, unroll=unroll)
    with jax.named_scope("own"):
        factor_ready(my_plane)
        arrived(my_plane)
        total = partial(my_plane)

    for step in range(parties):

        def sent(i, carry):
            lane = lax.rem(my_lane + i, lanes)
            piece = outgoing.at[step, lane]
            for plane in range(planes):
                pltpu.make_async_copy(
                    piece.at[plane], piece.at[plane], send_sem.at[step, lane, plane]
                ).wait()
            return carry

        lax.fori_loop(1 if step == parties - 1 else 0, lanes, sent, 0)

    def factor_sent(i, carry):
        h = remote(i)
        pltpu.make_async_copy(factor_out.at[h], factor_out.at[h], factor_send.at[h]).wait()
        if halves > 1:
            piece = factor_in.at[h, my_half]
            pltpu.make_async_copy(piece, piece, forward_send.at[h]).wait()
        return carry

    lax.fori_loop(0, planes - 1, factor_sent, 0)
    if halves > 1:
        piece = factor_out.at[my_plane]
        pltpu.make_async_copy(piece, piece, factor_send.at[my_plane]).wait()

    def add_part(i, sum_so_far):
        h = remote(planes - 2 - i)
        pltpu.make_async_copy(part_in.at[h], part_in.at[h], part_recv.at[h]).wait()
        return sum_so_far + part_in[h].astype(F32)

    with jax.named_scope("add_part"):
        total = lax.fori_loop(0, planes - 1, add_part, total, unroll=unroll)
        real, imag = total[:, :share], total[:, share:]
        intensity = real * real + imag * imag
        out_ref[...] = intensity
        peaks[me] = jnp.broadcast_to(jnp.max(intensity, axis=0, keepdims=True), peaks.shape[1:])

    def tell(i, carry):
        g = lax.rem(me + i, groups)
        pltpu.make_async_remote_copy(
            src_ref=peaks.at[me],
            dst_ref=peaks.at[me],
            send_sem=peak_send.at[g],
            recv_sem=peak_recv.at[me],
            device_id=(g, my_party),
            device_id_type=MESH,
        ).start()
        return carry

    lax.fori_loop(1, groups, tell, 0)

    def part_sent(i, carry):
        h = lax.rem(my_plane + i, planes)
        pltpu.make_async_copy(part_out.at[h], part_out.at[h], part_send.at[h]).wait()
        return carry

    lax.fori_loop(1, planes, part_sent, 0)

    def told(i, carry):
        g = lax.rem(me + i, groups)
        pltpu.make_async_copy(peaks.at[g], peaks.at[g], peak_recv.at[g]).wait()
        pltpu.make_async_copy(peaks.at[me], peaks.at[me], peak_send.at[g]).wait()
        return carry

    with jax.named_scope("told"):
        lax.fori_loop(1, groups, told, 0)
    peak_ref[...] = jnp.max(peaks[...], axis=0)[:1]


def finish(intensity_ref, peak_ref, out_ref, largest_ref):
    peak = peak_ref[...]
    out_ref[...] = intensity_ref[...] / (peak + 1.0)
    largest_ref[...] = peak


def solution(mesh):
    groups, parties = mesh.shape["src"], mesh.shape["grp"]
    lanes = math.gcd(groups, 2)
    planes = groups // lanes
    halves = math.gcd(parties, 2)

    def body(currents, leaf_basis, leaf_box, box_count, merge_factor, angle_factor):
        sources, width = currents.shape
        rank = leaf_basis.shape[1]
        leaves = box_count.shape[0]
        share = width // 2 // parties
        angles = angle_factor.shape[0]
        some = angles // halves
        hbm = pl.BlockSpec(memory_space=pl.ANY)
        vmem = pl.BlockSpec(memory_space=pltpu.VMEM)
        intensity, peak = pl.pallas_call(
            functools.partial(kernel, planes, lanes, parties, halves),
            out_shape=(
                jax.ShapeDtypeStruct((angles, share), F32),
                jax.ShapeDtypeStruct((1, share), F32),
            ),
            in_specs=[hbm] * 6,
            out_specs=(vmem, vmem),
            scratch_shapes=[
                pltpu.SMEM((leaves,), jnp.int32),
                pltpu.VMEM((1, sources), jnp.int32),
                pltpu.VMEM((2 * rank, sources), BF16),
                pltpu.VMEM((parties, sources, 2 * share), BF16),
                pltpu.VMEM(merge_factor.shape, BF16),
                pltpu.VMEM((some, *angle_factor.shape[1:]), BF16),
                pltpu.VMEM((2 * rank * leaves, sources), BF16),
                pltpu.VMEM((parties, lanes, planes, 2 * rank, share), BF16),
                pltpu.VMEM((parties, lanes, planes, 2 * rank, share), BF16),
                pltpu.VMEM((planes, 2 * some, parties * lanes * rank), BF16),
                pltpu.VMEM((planes, halves, 2 * some, parties * lanes * rank), BF16),
                pltpu.VMEM((planes, angles, 2 * share), BF16),
                pltpu.VMEM((planes, angles, 2 * share), BF16),
                pltpu.VMEM((groups, 8, share), F32),
                pltpu.SemaphoreType.DMA((5,)),
                pltpu.SemaphoreType.DMA((parties, 2)),
                pltpu.SemaphoreType.DMA((parties, lanes, planes)),
                pltpu.SemaphoreType.DMA((parties, lanes, planes)),
                pltpu.SemaphoreType.DMA((planes,)),
                pltpu.SemaphoreType.DMA((planes, halves)),
                pltpu.SemaphoreType.DMA((planes,)),
                pltpu.SemaphoreType.DMA((planes,)),
                pltpu.SemaphoreType.DMA((planes,)),
                pltpu.SemaphoreType.DMA((groups,)),
                pltpu.SemaphoreType.DMA((groups,)),
            ],
            compiler_params=pltpu.CompilerParams(
                collective_id=0, has_side_effects=True, vmem_limit_bytes=60 * 1024 * 1024
            ),
        )(
            box_count,
            leaf_box.reshape(1, sources),
            leaf_basis.reshape(2 * rank, sources),
            currents,
            merge_factor,
            angle_factor,
        )
        normalized, peak = pl.pallas_call(
            finish,
            out_shape=(
                jax.ShapeDtypeStruct((angles, share), F32),
                jax.ShapeDtypeStruct((1, share), F32),
            ),
            in_specs=[vmem, vmem],
            out_specs=(vmem, vmem),
        )(intensity, peak)
        return (normalized, peak.reshape(share))

    in_specs = (
        P(("src", "grp"), None),
        P(None, None, ("src", "grp")),
        P(("src", "grp")),
        P(("src", "grp")),
        P(None, None, ("src", "grp")),
        P("src", None, None, None),
    )
    out_specs = (P("src", "grp"), P("grp"))
    return jax.shard_map(body, mesh=mesh, in_specs=in_specs, out_specs=out_specs, check_vma=False)
```

```python
import functools
import math

import jax
import jax.numpy as jnp
from jax import lax
from jax.experimental import pallas as pl
from jax.experimental.pallas import tpu as pltpu
from jax.sharding import PartitionSpec as P

MESH = pl.DeviceIdType.MESH
F32 = jnp.float32
BF16 = jnp.bfloat16


def kernel(
    planes, lanes, parties, halves, count_hbm, box_hbm, basis_hbm, currents_hbm, merge_hbm, angle_hbm,
    out_ref, peak_ref,
    count_ref, box_ref, basis, x, merge, angle, left, outgoing, received, factor_out, factor_in, part_out, part_in,
    peaks,
    load_sem, x_sem, send_sem, recv_sem, factor_send, factor_recv, beside_recv, forward_send, part_send, part_recv,
    peak_send, peak_recv,
):
    me = lax.axis_index("src")
    my_plane, my_lane = me // lanes, lax.rem(me, lanes)
    my_party = lax.axis_index("grp")
    my_half = lax.rem(my_party, halves)
    partner = my_party + (halves - 1) * (1 - 2 * my_half)
    groups = planes * lanes
    peers = lanes * parties
    rank = merge.shape[1] // groups
    leaves = count_ref.shape[0]
    share = x.shape[2] // 2
    excite = currents_hbm.shape[1] // 2
    some = angle.shape[0]
    angles = some * halves
    split = 2 if leaves % 2 == 0 else 1
    unroll = planes <= 8

    load_basis = pltpu.make_async_copy(basis_hbm, basis, load_sem.at[0])
    load_basis.start()
    load_box = pltpu.make_async_copy(box_hbm, box_ref, load_sem.at[1])
    load_box.start()
    load_count = pltpu.make_async_copy(count_hbm, count_ref, load_sem.at[2])
    load_count.start()
    load_angle = pltpu.make_async_copy(angle_hbm.at[pl.ds(my_half * some, some)], angle, load_sem.at[3])
    load_merge = pltpu.make_async_copy(merge_hbm, merge, load_sem.at[4])
    for step in range(parties):
        quarter = lax.rem(my_party + 1 + step, parties)
        for part in range(2):
            start = pl.multiple_of(part * excite + quarter * share, 128)
            pltpu.make_async_copy(
                currents_hbm.at[:, pl.ds(start, share)],
                x.at[step, :, pl.ds(part * share, share)],
                x_sem.at[step],
            ).start()
        if step == 0:
            load_angle.start()
            load_merge.start()

    barrier = pltpu.get_barrier_semaphore()

    def peer(i):
        other = lax.rem(my_lane * parties + my_party + i, peers)
        return other // parties, lax.rem(other, parties)

    def greet(i, carry):
        lane, party = peer(i)
        pl.semaphore_signal(
            barrier, inc=1, device_id=(my_plane * lanes + lane, party), device_id_type=MESH
        )
        return carry

    lax.fori_loop(1, peers, greet, 0)

    def greet_far(i, carry):
        plane = lax.rem(my_plane + 1 + i // lanes, planes)
        pl.semaphore_signal(
            barrier,
            inc=1,
            device_id=(plane * lanes + lax.rem(i, lanes), my_party),
            device_id_type=MESH,
        )
        return carry

    lax.fori_loop(0, (planes - 1) * lanes, greet_far, 0)

    def remote(i):
        upper = lax.rem(my_plane // ((planes + 1) // 2), 2)
        down = planes - 1 - i
        down = down - (my_plane - down + planes) // planes
        up = i + (i - my_plane + planes) // planes
        return (1 - upper) * down + upper * up

    def relay_factor():
        wide = [angle[:, q].astype(F32) for q in range(parties)]
        span = lanes * rank
        for h in range(planes):
            rows = [
                jnp.concatenate([wide[q][:, p, h * span : (h + 1) * span] for q in range(parties)], axis=1)
                for p in range(2)
            ]
            factor_out[h] = jnp.concatenate(rows, axis=0).astype(BF16)

    def share_factor(i, carry):
        h = remote(i)
        pltpu.make_async_remote_copy(
            src_ref=factor_out.at[h],
            dst_ref=factor_in.at[my_half, my_plane],
            send_sem=factor_send.at[0],
            recv_sem=factor_recv.at[my_plane],
            device_id=(h * lanes + my_lane, my_party),
            device_id_type=MESH,
        ).start()
        return carry

    def share_beside():
        if halves > 1:
            pltpu.make_async_remote_copy(
                src_ref=factor_out.at[my_plane],
                dst_ref=factor_in.at[my_half, my_plane],
                send_sem=factor_send.at[0],
                recv_sem=beside_recv.at[0],
                device_id=(me, partner),
                device_id_type=MESH,
            ).start()
        factor_in[my_half, my_plane] = factor_out[my_plane]

    with jax.named_scope("wait_basis"):
        load_basis.wait()
        load_box.wait()
        load_count.wait()
    with jax.named_scope("left_build"):
        box = box_ref[...]
        count = jnp.zeros(box.shape, F32)
        for b in range(leaves):
            count = jnp.where(box == b, count_ref[b].astype(F32), count)
        scale = lax.rsqrt(jnp.maximum(count, 1.0))
        scaled = (basis[...].astype(F32) * scale).astype(BF16)
        for b in range(leaves):
            member = (box == b).astype(F32).astype(BF16)
            left[2 * rank * b : 2 * rank * (b + 1), :] = scaled * member

    def send(step, lane, plane):
        quarter = lax.rem(my_party + 1 + step, parties)
        pltpu.make_async_remote_copy(
            src_ref=outgoing.at[step, lane, plane],
            dst_ref=received.at[plane, my_party * lanes + my_lane],
            send_sem=send_sem.at[step // (parties - 1)],
            recv_sem=recv_sem.at[plane],
            device_id=(my_plane * lanes + lane, quarter),
            device_id_type=MESH,
        ).start()

    block = math.gcd(groups, 8)
    for step in range(parties):
        with jax.named_scope(f"xwait{step}"):
            pltpu.make_async_copy(x.at[step], x.at[step], x_sem.at[step]).wait()
            if step == 0:
                load_angle.wait()
                load_merge.wait()
        with jax.named_scope(f"leaf{step}"):
            chunks = []
            depth = leaves // split
            for c in range(split):
                rows = slice(2 * rank * depth * c, 2 * rank * depth * (c + 1))
                raw = jnp.dot(left[rows, :], x[step], preferred_element_type=F32)
                reals, imags = [], []
                for b in range(depth):
                    top = raw[2 * rank * b : 2 * rank * b + rank]
                    low = raw[2 * rank * b + rank : 2 * rank * (b + 1)]
                    reals.append(top[:, :share] - low[:, share:])
                    imags.append(top[:, share:] + low[:, :share])
                chunks.append(
                    jnp.concatenate(
                        [jnp.concatenate(reals, axis=0), jnp.concatenate(imags, axis=0)], axis=1
                    )
                )
            leaf = jnp.concatenate(chunks, axis=0).astype(BF16)
            if step == 0:
                relay_factor()
            for first in range(0, groups, block):
                rows = slice(first * rank, (first + block) * rank)
                one = jnp.dot(merge[0, rows, :], leaf, preferred_element_type=F32)
                two = jnp.dot(merge[1, rows, :], leaf, preferred_element_type=F32)
                real = (one[:, :share] - two[:, share:]).astype(BF16)
                imag = (one[:, share:] + two[:, :share]).astype(BF16)
                for g in range(block):
                    cut = slice(g * rank, (g + 1) * rank)
                    plane, lane = divmod(first + g, lanes)
                    outgoing[step, lane, plane, :rank] = real[cut]
                    outgoing[step, lane, plane, rank:] = imag[cut]
        if step == 0:
            with jax.named_scope("barrier"):
                pl.semaphore_wait(barrier, peers - 1 + (planes - 1) * lanes)
            lax.fori_loop(0, planes - 1, share_factor, 0)
            share_beside()
        own = 1 if step == parties - 1 else 0

        def send_plane(i, carry):
            plane = remote(i)

            def send_lane(j, inner):
                send(step, lax.rem(my_lane + j, lanes), plane)
                return inner

            return lax.fori_loop(own, lanes, send_lane, carry)

        lax.fori_loop(0, planes - 1, send_plane, 0)

    for step in range(parties):

        def send_home(j, carry):
            send(step, lax.rem(my_lane + j, lanes), my_plane)
            return carry

        lax.fori_loop(1 if step == parties - 1 else 0, lanes, send_home, 0)
    for plane in range(planes):
        received[plane, my_party * lanes + my_lane] = outgoing[parties - 1, my_lane, plane]

    with jax.named_scope("forward"):

        def forward(i, carry):
            h = remote(planes - 2 - i)
            piece = factor_in.at[my_half, h]
            pltpu.make_async_copy(piece, piece, factor_recv.at[h]).wait()
            if halves > 1:
                pltpu.make_async_remote_copy(
                    src_ref=piece,
                    dst_ref=piece,
                    send_sem=forward_send.at[0],
                    recv_sem=beside_recv.at[0],
                    device_id=(me, partner),
                    device_id_type=MESH,
                ).start()
            return carry

        lax.fori_loop(0, planes - 1, forward, 0)

    def arrived(h):
        pieces = received.at[h, pl.ds(0, peers - 1)]
        pltpu.make_async_copy(pieces, pieces, recv_sem.at[h]).wait()

    def partial(h):
        pieces = [
            received[h, k].astype(F32) for k in range(peers)
        ]
        coefs = jnp.concatenate(
            [
                jnp.concatenate([piece[:rank] for piece in pieces], axis=0),
                jnp.concatenate([piece[rank:] for piece in pieces], axis=0),
            ],
            axis=1,
        ).astype(BF16)
        reals, imags = [], []
        factor = jnp.concatenate([factor_in[k, h] for k in range(halves)], axis=0)
        total = jnp.dot(factor, coefs, preferred_element_type=F32)
        for k in range(halves):
            top = total[2 * some * k : 2 * some * k + some]
            low = total[2 * some * k + some : 2 * some * (k + 1)]
            reals.append(top[:, :share] - low[:, share:])
            imags.append(top[:, share:] + low[:, :share])
        return jnp.concatenate(
            [jnp.concatenate(reals, axis=0), jnp.concatenate(imags, axis=0)], axis=1
        )

    def pass_on(i, carry):
        h = remote(i)
        arrived(h)
        part_out[h] = partial(h).astype(BF16)
        pltpu.make_async_remote_copy(
            src_ref=part_out.at[h],
            dst_ref=part_in.at[my_plane],
            send_sem=part_send.at[0],
            recv_sem=part_recv.at[0],
            device_id=(h * lanes + my_lane, my_party),
            device_id_type=MESH,
        ).start()
        return carry

    with jax.named_scope("beside"):
        if halves > 1:
            other = factor_in.at[1 - my_half]
            pltpu.make_async_copy(other, other, beside_recv.at[0]).wait()
    with jax.named_scope("pass_on"):
        lax.fori_loop(0, planes - 1, pass_on, 0, unroll=unroll)
    with jax.named_scope("own"):
        arrived(my_plane)
        total = partial(my_plane)

    def drained(ref, sem):
        pltpu.make_async_copy(ref, ref, sem).wait()

    drained(outgoing.at[pl.ds(0, parties - 1)], send_sem.at[0])
    if lanes > 1:
        drained(outgoing.at[parties - 1, pl.ds(0, lanes - 1)], send_sem.at[1])
    if halves > 1:
        drained(factor_out, factor_send.at[0])
        drained(factor_in.at[my_half, pl.ds(0, planes - 1)], forward_send.at[0])
    else:
        drained(factor_out.at[pl.ds(0, planes - 1)], factor_send.at[0])

    def add_part(i, sum_so_far):
        return sum_so_far + part_in[remote(planes - 2 - i)].astype(F32)

    with jax.named_scope("add_part"):
        parts = part_in.at[pl.ds(0, planes - 1)]
        drained(parts, part_recv.at[0])
        total = lax.fori_loop(0, planes - 1, add_part, total, unroll=unroll)
        real, imag = total[:, :share], total[:, share:]
        intensity = real * real + imag * imag
        out_ref[...] = intensity
        peaks[me] = jnp.broadcast_to(jnp.max(intensity, axis=0, keepdims=True), peaks.shape[1:])

    def tell(i, carry):
        g = lax.rem(me + i, groups)
        pltpu.make_async_remote_copy(
            src_ref=peaks.at[me],
            dst_ref=peaks.at[me],
            send_sem=peak_send.at[0],
            recv_sem=peak_recv.at[0],
            device_id=(g, my_party),
            device_id_type=MESH,
        ).start()
        return carry

    lax.fori_loop(1, groups, tell, 0)

    drained(part_out.at[pl.ds(0, planes - 1)], part_send.at[0])
    with jax.named_scope("told"):
        others = peaks.at[pl.ds(0, groups - 1)]
        drained(others, peak_recv.at[0])
        drained(others, peak_send.at[0])
    peak_ref[...] = jnp.max(peaks[...], axis=0)[:1]


def finish(intensity_ref, peak_ref, out_ref, largest_ref):
    peak = peak_ref[...]
    out_ref[...] = intensity_ref[...] / (peak + 1.0)
    largest_ref[...] = peak


def solution(mesh):
    groups, parties = mesh.shape["src"], mesh.shape["grp"]
    lanes = math.gcd(groups, 2)
    planes = groups // lanes
    halves = math.gcd(parties, 2)

    def body(currents, leaf_basis, leaf_box, box_count, merge_factor, angle_factor):
        sources, width = currents.shape
        rank = leaf_basis.shape[1]
        leaves = box_count.shape[0]
        share = width // 2 // parties
        angles = angle_factor.shape[0]
        some = angles // halves
        hbm = pl.BlockSpec(memory_space=pltpu.HBM)
        vmem = pl.BlockSpec(memory_space=pltpu.VMEM)
        intensity, peak = pl.pallas_call(
            functools.partial(kernel, planes, lanes, parties, halves),
            out_shape=(pltpu.VMEM((angles, share), F32), pltpu.VMEM((1, share), F32)),
            in_specs=[hbm] * 6,
            out_specs=(vmem, vmem),
            scratch_shapes=[
                pltpu.SMEM((leaves,), jnp.int32),
                pltpu.VMEM((1, sources), jnp.int32),
                pltpu.VMEM((2 * rank, sources), BF16),
                pltpu.VMEM((parties, sources, 2 * share), BF16),
                pltpu.VMEM(merge_factor.shape, BF16),
                pltpu.VMEM((some, *angle_factor.shape[1:]), BF16),
                pltpu.VMEM((2 * rank * leaves, sources), BF16),
                pltpu.VMEM((parties, lanes, planes, 2 * rank, share), BF16),
                pltpu.VMEM((planes, parties * lanes, 2 * rank, share), BF16),
                pltpu.VMEM((planes, 2 * some, parties * lanes * rank), BF16),
                pltpu.VMEM((halves, planes, 2 * some, parties * lanes * rank), BF16),
                pltpu.VMEM((planes, angles, 2 * share), BF16),
                pltpu.VMEM((planes, angles, 2 * share), BF16),
                pltpu.VMEM((groups, 8, share), F32),
                pltpu.SemaphoreType.DMA((5,)),
                pltpu.SemaphoreType.DMA((parties,)),
                pltpu.SemaphoreType.DMA((2,)),
                pltpu.SemaphoreType.DMA((planes,)),
                pltpu.SemaphoreType.DMA((1,)),
                pltpu.SemaphoreType.DMA((planes,)),
                pltpu.SemaphoreType.DMA((1,)),
                pltpu.SemaphoreType.DMA((1,)),
                pltpu.SemaphoreType.DMA((1,)),
                pltpu.SemaphoreType.DMA((1,)),
                pltpu.SemaphoreType.DMA((1,)),
                pltpu.SemaphoreType.DMA((1,)),
            ],
            compiler_params=pltpu.CompilerParams(
                collective_id=0, has_side_effects=True, vmem_limit_bytes=60 * 1024 * 1024
            ),
        )(
            box_count,
            leaf_box.reshape(1, sources),
            leaf_basis.reshape(2 * rank, sources),
            currents,
            merge_factor,
            angle_factor,
        )
        intensity = pltpu.with_memory_space_constraint(intensity, pltpu.VMEM)
        peak = pltpu.with_memory_space_constraint(peak, pltpu.VMEM)
        normalized, peak = pl.pallas_call(
            finish,
            out_shape=(
                jax.ShapeDtypeStruct((angles, share), F32),
                jax.ShapeDtypeStruct((1, share), F32),
            ),
            in_specs=[vmem, vmem],
            out_specs=(vmem, vmem),
        )(intensity, peak)
        return (normalized, peak.reshape(share))

    in_specs = (
        P(("src", "grp"), None),
        P(None, None, ("src", "grp")),
        P(("src", "grp")),
        P(("src", "grp")),
        P(None, None, ("src", "grp")),
        P("src", None, None, None),
    )
    out_specs = (P("src", "grp"), P("grp"))
    return jax.shard_map(body, mesh=mesh, in_specs=in_specs, out_specs=out_specs, check_vma=False)
```
